32 devices in a mesh: dp: 4 (over y, x), sp: 4 (over z), shift: 2 (over core).
Axes of the slice: x: 2, y: 2, z: 4, core: 2. Of those that a mesh axis runs over, the one named last changes fastest.
Arguments:
- query_rows: bfloat16 [8, 1024, 32, 128], P(('shift', 'dp'), 'sp'), parts along dimension 0, may hold values from -6 to 6
- key_rows: bfloat16 [8, 1024, 32, 128], P(('shift', 'dp'), 'sp'), parts along dimension 0, may hold values from -6 to 6
- value_rows: bfloat16 [8, 1024, 32, 128], P(('shift', 'dp'), 'sp'), parts along dimension 0, may hold values from -6 to 6
- out_weight: bfloat16 [8192, 4096], P(('shift', 'dp')), parts along dimension 0, may hold values from -0.09375 to 0.09375
Outputs:
- mixer_out: bfloat16 [8, 1024, 4096], P(('shift', 'dp'), 'sp'), parts along dimension 0
The draws below stay inside these ranges and needn't reach their ends.
There are 2 independent parts, one for each index of `shift`. The reference program is written for one: setup_inputs(seed, part) draws one part's arguments, and reference() takes and returns one part's arrays. A program takes and returns all parts, laid end to end along the dimension named above; each array names one. Nothing has to cross between parts.
All inputs are finite; a program needn't handle non-finite values.
Results may differ from the reference program's by a relative error of at most 0.006.
Values may be sent and summed in bfloat16 or wider, within the bound.
A program may use at most 128 MiB of HBM per device.

```python
import jax
import jax.numpy as jnp
from jax import lax

HEADS = 32
HEAD_SIZE = 128
BATCH = 4
TOKENS = 1024
WIDTH = 4096


def steps_of(key, shape, shards, least, top_value):
    factor_of = 1.0
    for dim, shards_of in shards:
        steps = jax.random.uniform(jax.random.fold_in(jax.random.fold_in(key, 6), dim), (shards_of,), jnp.float32, least / len(shards), top_value / len(shards))
        factor_of = factor_of * jnp.repeat(jnp.exp(steps), shape[dim] // shards_of).reshape((-1,) + (1,) * (len(shape) - 1 - dim))
    return factor_of


def noise(key, dims, scale, most, cuts=(), dtype=jnp.bfloat16):
    entries = jax.random.normal(key, dims, jnp.float32) * scale
    if len(cuts) > 0:
        entries = steps_of(key, dims, cuts, -0.22, 0.18) * entries
    return jnp.clip(entries, min=-most, max=most).astype(dtype)


def setup_inputs(seed: int = 0, part: int = 0) -> dict:
    key_of = jax.random.split(jax.random.key(seed), 5)
    own_keys = jax.random.split(jax.random.fold_in(key_of[4], part), 5)
    return {
        "query_rows": noise(own_keys[0], (BATCH, TOKENS, HEADS, HEAD_SIZE), 1.0, 6.0, ((0, 4), (1, 4))),
        "key_rows": noise(own_keys[1], (BATCH, TOKENS, HEADS, HEAD_SIZE), 1.0, 6.0, ((0, 4), (1, 4))),
        "value_rows": noise(own_keys[2], (BATCH, TOKENS, HEADS, HEAD_SIZE), 1.0, 6.0, ((0, 4), (1, 4))),
        "out_weight": noise(own_keys[3], (WIDTH, WIDTH), WIDTH ** -0.5, 0.09375, ((0, 4),)),
    }


def feature_map(values):
    wide = values.astype(jnp.float32)
    return (jnp.where(wide > 0.0, wide + 1.0, jnp.exp(jnp.minimum(wide, 0.0)))).astype(jnp.bfloat16)


def finish_heads(read, count):
    result = read * count ** 0.5
    return result.astype(jnp.bfloat16)


def ask_state(features, state, mass):
    small = lax.optimization_barrier(state.astype(jnp.bfloat16))
    top = jnp.einsum("bthd,bhde->bthe", features.astype(jnp.float32), small.astype(jnp.float32))
    bottom = jnp.einsum("bthd,bhd->bth", features.astype(jnp.float32), mass, precision=lax.Precision.HIGHEST)
    return top / (bottom + 1e-3)[..., None]


def reference(query_rows, key_rows, value_rows, out_weight):
    query_feature, key_feature = lax.optimization_barrier((feature_map(query_rows), feature_map(key_rows)))
    state = jnp.einsum("bthd,bthe->bhde", key_feature.astype(jnp.float32), value_rows.astype(jnp.float32)) / TOKENS
    mass = jnp.sum(key_feature.astype(jnp.float32), axis=1) / TOKENS
    mixed = finish_heads(ask_state(query_feature, state, mass), TOKENS).reshape(BATCH, TOKENS, WIDTH)
    mixed = lax.optimization_barrier(mixed)
    mixer_out = jnp.einsum("btw,wv->btv", mixed.astype(jnp.float32), out_weight.astype(jnp.float32)).astype(jnp.bfloat16)
    return mixer_out
```

```python
import functools

import jax
import jax.numpy as jnp
from jax import lax
from jax.experimental import pallas as pl
from jax.experimental.pallas import tpu as pltpu
from jax.sharding import PartitionSpec as P


def feature_map(values):
    wide = values.astype(jnp.float32)
    return jnp.where(wide > 0.0, wide + 1.0, jnp.exp(jnp.minimum(wide, 0.0))).astype(jnp.bfloat16)


def plain_body(query_rows, key_rows, value_rows, out_weight):
    query_feature, key_feature = (feature_map(query_rows), feature_map(key_rows))
    count = query_rows.shape[1] * lax.axis_size("sp")
    state = (
        jnp.einsum("bthd,bthe->bhde", key_feature, value_rows, preferred_element_type=jnp.float32)
        / count
    )
    mass = jnp.sum(key_feature.astype(jnp.float32), axis=1) / count
    state = lax.psum(state.astype(jnp.bfloat16), "sp")
    mass = lax.psum(mass, "sp")
    top = jnp.einsum("bthd,bhde->bthe", query_feature, state, preferred_element_type=jnp.float32)
    bottom = jnp.einsum(
        "bthd,bhd->bth", query_feature.astype(jnp.float32), mass, precision=lax.Precision.HIGHEST
    )
    mixed = (top / (bottom + 0.001)[..., None] * count**0.5).astype(jnp.bfloat16)
    mixed = mixed.reshape(mixed.shape[0], mixed.shape[1], -1)
    mine = lax.all_to_all(mixed, "dp", split_axis=2, concat_axis=0, tiled=True)
    part = jnp.einsum("btw,wv->btv", mine, out_weight, preferred_element_type=jnp.float32)
    return lax.psum_scatter(part.astype(jnp.bfloat16), "dp", scatter_dimension=0, tiled=True)


MESH = pl.DeviceIdType.MESH
NT = (((1,), (1,)), ((), ()))
TN = (((0,), (0,)), ((), ()))
EXTRA = 16
PART = 4


def feature32(values):
    wide = values.astype(jnp.float32)
    return jnp.where(wide > 0.0, wide + 1.0, jnp.exp(jnp.minimum(wide, 0.0)))


def remote(src, dst, send, recv, **where):
    return pltpu.make_async_remote_copy(
        src_ref=src, dst_ref=dst, send_sem=send, recv_sem=recv, device_id=where, device_id_type=MESH
    )


def kernel(
    NS, count, q_hbm, k_hbm, v_hbm, w_hbm, out_hbm,
    kin, vin, qin, wide, wide2, w, own, up, inb, cb, sall, qf, mixed,
    m1, r1, s2, r2, keep, outv,
    ksem, vsem, lsem, wsem, osem, qs, qr, us, inr, cbr, ds, sts, str_, s1, t1, s2s, s2r,
):
    d, p = lax.axis_index("dp"), lax.axis_index("sp")
    i, j = lax.div(d, 2), lax.rem(d, 2)
    T, HD, size = kin.shape[1:]
    G, SUB = up.shape[0], sall.shape[1]
    NC, C = keep.shape[0], keep.shape[2]
    half, mid = NC // 2, NS // 2

    def peer(r):
        return lax.rem(i + r // 2, 2) * 2 + lax.rem(j + r % 2, 2)

    left = p < mid
    side = 1 - lax.div(p, mid)
    center = p - 1 + 2 * side
    outer = p + 1 - 2 * side
    is_mid = jnp.logical_or(p == mid - 1, p == mid)
    has_outer = jnp.logical_and(p > 0, p < NS - 1)
    has_inner = jnp.logical_not(is_mid)

    loads = {}
    for n in range(4):
        rows = pl.ds(peer((n + 1) % 4) * HD, HD)
        loads[n] = (
            pltpu.make_async_copy(k_hbm.at[:, rows], kin.at[n], ksem.at[n]),
            pltpu.make_async_copy(v_hbm.at[:, rows], vin.at[n], vsem.at[n]),
        )
        loads[n][0].start()
        loads[n][1].start()

    barrier = pltpu.get_barrier_semaphore()
    for r in (1, 2, 3):
        pl.semaphore_signal(barrier, inc=1, device_id={"dp": peer(r)}, device_id_type=MESH)
    pl.semaphore_signal(barrier, inc=1, device_id={"sp": center}, device_id_type=MESH)

    @pl.when(has_outer)
    def _():
        pl.semaphore_signal(barrier, inc=1, device_id={"sp": outer}, device_id_type=MESH)
        pl.semaphore_wait(barrier, 5)

    @pl.when(jnp.logical_not(has_outer))
    def _():
        pl.semaphore_wait(barrier, 4)

    queries = {}
    for r in (1, 2, 3):
        rows = pl.ds(peer(r) * HD, HD)
        queries[r] = remote(q_hbm.at[:, rows], qin.at[r], qs.at[r], qr.at[r], dp=peer(r))
        queries[r].start()
    own_query = pltpu.make_async_copy(q_hbm.at[:, pl.ds(d * HD, HD)], qin.at[0], lsem)
    own_query.start()
    weights = pltpu.make_async_copy(w_hbm, w, wsem)
    weights.start()

    def widen(src, dst, fn):
        step = 64

        @pl.loop(0, T // step)
        def _(x):
            block = fn(src[pl.ds(pl.multiple_of(x * step, step), step)])
            rows = step * HD
            dst[pl.ds(pl.multiple_of(x * rows, rows), rows)] = block.reshape(rows, size)

    def up_end(g):
        return remote(up.at[g], inb.at[g], us.at[g], inr.at[g], sp=center)

    def up_mid(g):
        return remote(up.at[g], cb.at[g], us.at[g], cbr.at[g], sp=center)

    def down(g):
        return remote(cb.at[g], cb.at[g], ds.at[g], cbr.at[g], sp=outer)

    def spread(g):
        n, x = lax.div(g, SUB), lax.rem(g, SUB)
        r = lax.rem(n + 1, 4)
        dd = lax.rem(i + lax.div(r, 2), 2) * 2 + lax.rem(j + lax.rem(r, 2), 2)
        return remote(cb.at[g], sall.at[n, x], sts.at[g], str_.at[n, x], dp=dd)

    for n in range(4):
        loads[n][0].wait()
        loads[n][1].wait()
        widen(kin.at[n], wide, feature32)
        widen(vin.at[n], wide2, lambda x: x.astype(jnp.float32))

        @pl.loop(0, SUB)
        def _(x):
            g = n * SUB + x
            row = lax.broadcasted_iota(jnp.int32, (EXTRA, size), 0)
            masses = jnp.zeros((EXTRA, size), jnp.float32)
            for k in range(PART):
                key = wide[pl.ds(x * PART + k, T, stride=HD), :].astype(jnp.bfloat16)
                value = wide2[pl.ds(x * PART + k, T, stride=HD), :].astype(jnp.bfloat16)
                state = lax.dot_general(value, key, TN, preferred_element_type=jnp.float32) / count
                mass = jnp.sum(key.astype(jnp.float32), axis=0, keepdims=True) / count
                masses = jnp.where(row == k, mass, masses)
                own[g, k * size : (k + 1) * size] = state
                up[g, k * size : (k + 1) * size] = state.astype(up.dtype)
            own[g, PART * size :] = masses
            up[g, PART * size :] = masses.astype(up.dtype)

            @pl.when(has_inner)
            def _():
                up_end(g).start()

    def take_in(g):
        up_end(g).wait_recv()
        total = own[g] + inb[g].astype(jnp.float32)
        own[g] = total
        up[g] = total.astype(up.dtype)
        up_mid(g).start()

    def finish(g):
        up_mid(g).wait_recv()

        @pl.when(is_mid)
        def _():
            cb[g] = (own[g] + cb[g].astype(jnp.float32)).astype(cb.dtype)

        @pl.when(has_outer)
        def _():
            down(g).start()

    LAG = min(2, SUB)

    def reduce_states(first, last, send):
        @pl.when(is_mid)
        def _():
            for g in range(first, min(first + LAG, last)):
                take_in(g)

        @pl.loop(first, last)
        def _(g):
            @pl.when(jnp.logical_and(is_mid, g + LAG < last))
            def _():
                take_in(g + LAG)

            finish(g)
            if send:
                spread(g).start()

    def query_features(r):
        widen(qin.at[r], wide, feature32)
        for k in range(HD):
            qf[r, k] = wide[pl.ds(k, T, stride=HD), :].astype(qf.dtype)

    def mix(r, states):
        for k in range(HD):
            x, kk = k // PART, k % PART
            block = states(x)
            masses = block[PART * size :].astype(jnp.float32)
            mass = jnp.broadcast_to(masses[kk : kk + 1], (size, size)).astype(jnp.bfloat16)
            both = jnp.concatenate([block[kk * size : (kk + 1) * size], mass], axis=0)
            read = lax.dot_general(qf[r, k], both, NT, preferred_element_type=jnp.float32)
            read = read[:, :size] / (read[:, size:] + 0.001) * count**0.5
            mixed[r, :, k * size : (k + 1) * size] = read.astype(mixed.dtype)

    def wait_spread(n):
        for x in range(SUB):
            remote(cb.at[0], sall.at[n, x], sts.at[0], str_.at[n, x], dp=d).wait_recv()

    def columns(c, odd):
        return pl.ds(pl.multiple_of((2 * c + odd) * C, C), C)

    def first(c, odd, diagonal):
        return remote(
            m1.at[odd, c, diagonal], r1.at[odd, c, diagonal], s1.at[odd, c, diagonal], t1.at[odd, c, diagonal],
            dp=peer(2 if odd else 1),
        )

    def second(c, odd):
        return remote(s2.at[odd, c], r2.at[odd, c], s2s.at[odd, c], s2r.at[odd, c], dp=peer(1 if odd else 2))

    def times(r, c, odd):
        return jnp.dot(mixed[r], w[:, columns(c, odd)], preferred_element_type=jnp.float32)

    reduce_states(0, 3 * SUB, True)
    for r in (1, 2):
        queries[r].wait_recv()
        query_features(r)
    for r in (1, 2):
        wait_spread(r - 1)
        mix(r, lambda x: sall[r - 1, x])
    weights.wait()

    @pl.loop(0, half)
    def _(c):
        for odd in range(2):
            m1[odd, c, 0] = times(2 if odd else 1, c, odd).astype(m1.dtype)
            first(c, odd, 0).start()

    queries[3].wait_recv()
    query_features(3)
    reduce_states(3 * SUB, 4 * SUB, False)
    wait_spread(2)
    mix(3, lambda x: sall[2, x])

    @pl.loop(0, half)
    def _(c):
        for odd in range(2):
            m1[odd, c, 1] = times(3, c, odd).astype(m1.dtype)
            first(c, odd, 1).start()

    own_query.wait()
    query_features(0)
    mix(0, lambda x: cb[3 * SUB + x])

    @pl.loop(0, half)
    def _(c):
        for odd in range(2):
            block = times(0, c, odd)
            first(c, odd, 0).wait_recv()
            keep[2 * c + odd] = block + r1[odd, c, 0].astype(jnp.float32)

    @pl.loop(0, half)
    def _(c):
        for odd in range(2):
            block = times(1 if odd else 2, c, odd)
            first(c, odd, 1).wait_recv()
            s2[odd, c] = (block + r1[odd, c, 1].astype(jnp.float32)).astype(s2.dtype)
            second(c, odd).start()

    def leave(c, odd):
        return pltpu.make_async_copy(outv.at[2 * c + odd], out_hbm.at[:, columns(c, odd)], osem.at[2 * c + odd])

    @pl.loop(0, half)
    def _(c):
        for odd in range(2):
            second(c, odd).wait_recv()
            outv[2 * c + odd] = (keep[2 * c + odd] + r2[odd, c].astype(jnp.float32)).astype(outv.dtype)
            leave(c, odd).start()

    for r in (1, 2, 3):
        queries[r].wait_send()

    @pl.loop(0, G)
    def _(g):
        up_end(g).wait_send()

        @pl.when(has_outer)
        def _():
            down(g).wait_send()

    @pl.loop(0, 3 * SUB)
    def _(g):
        spread(g).wait_send()

    @pl.loop(0, half)
    def _(c):
        for odd in range(2):
            first(c, odd, 0).wait_send()
            first(c, odd, 1).wait_send()
            second(c, odd).wait_send()
            leave(c, odd).wait()


def kernel_body(query_rows, key_rows, value_rows, out_weight):
    NS = lax.axis_size("sp")
    _, T, H, size = query_rows.shape
    V, rows = out_weight.shape[1], out_weight.shape[0]
    HD, NC = H // 4, 16
    C, half, count = V // NC, NC // 2, T * NS
    SUB = HD // PART
    G, R = 4 * SUB, PART * size + EXTRA
    bf, f32 = jnp.bfloat16, jnp.float32
    dma = pltpu.SemaphoreType.DMA
    hbm = pl.BlockSpec(memory_space=pl.ANY)
    out = pl.pallas_call(
        functools.partial(kernel, NS, count),
        out_shape=jax.ShapeDtypeStruct((T, V), bf),
        in_specs=[hbm] * 4,
        out_specs=hbm,
        scratch_shapes=[
            pltpu.VMEM((4, T, HD, size), bf),
            pltpu.VMEM((4, T, HD, size), bf),
            pltpu.VMEM((4, T, HD, size), bf),
            pltpu.VMEM((T * HD, size), f32),
            pltpu.VMEM((T * HD, size), f32),
            pltpu.VMEM((rows, V), bf),
            pltpu.VMEM((G, R, size), f32),
            pltpu.VMEM((G, R, size), bf),
            pltpu.VMEM((G, R, size), bf),
            pltpu.VMEM((G, R, size), bf),
            pltpu.VMEM((3, SUB, R, size), bf),
            pltpu.VMEM((4, HD, T, size), bf),
            pltpu.VMEM((4, T, rows), bf),
            pltpu.VMEM((2, half, 2, T, C), bf),
            pltpu.VMEM((2, half, 2, T, C), bf),
            pltpu.VMEM((2, half, T, C), bf),
            pltpu.VMEM((2, half, T, C), bf),
            pltpu.VMEM((NC, T, C), f32),
            pltpu.VMEM((NC, T, C), bf),
            dma((4,)), dma((4,)), dma, dma, dma((NC,)), dma((4,)), dma((4,)),
            dma((G,)), dma((G,)), dma((G,)), dma((G,)), dma((3 * SUB,)), dma((3, SUB)),
            dma((2, half, 2)), dma((2, half, 2)), dma((2, half)), dma((2, half)),
        ],
        compiler_params=pltpu.CompilerParams(
            collective_id=0, has_side_effects=True, vmem_limit_bytes=60 * 2**20
        ),
    )(query_rows[0], key_rows[0], value_rows[0], out_weight)
    return out[None]


def split_of(n):
    for a in range(int(n**0.5), 0, -1):
        if n % a == 0:
            return a, n // a


def body(query_rows, key_rows, value_rows, out_weight):
    ND, NS = lax.axis_size("dp"), lax.axis_size("sp")
    batch, T, H, size = query_rows.shape
    rows, V = out_weight.shape
    fits = batch == 1 and split_of(ND) == (2, 2) and NS == 4 and H % 4 == 0 and (H // 4) % 8 == 0
    fits = fits and size == 128 and T % 64 == 0 and V % 4096 == 0 and rows * 4 == H * size
    need = 2 * rows * V + 18 * T * V + 12 * T * H * size + 14 * H * size * size
    run = kernel_body if fits and need < 50 * 2**20 else plain_body
    return run(query_rows, key_rows, value_rows, out_weight)


def solution(mesh):
    placed = (
        P(("shift", "dp"), "sp", None, None),
        P(("shift", "dp"), "sp", None, None),
        P(("shift", "dp"), "sp", None, None),
        P(("shift", "dp"), None),
    )
    return jax.shard_map(
        body, mesh=mesh, in_specs=placed, out_specs=P(("shift", "dp"), "sp", None), check_vma=False
    )
```

```python
import functools

import jax
import jax.numpy as jnp
from jax import lax
from jax.experimental import pallas as pl
from jax.experimental.pallas import tpu as pltpu
from jax.sharding import PartitionSpec as P


def feature_map(values):
    wide = values.astype(jnp.float32)
    return jnp.where(wide > 0.0, wide + 1.0, jnp.exp(jnp.minimum(wide, 0.0))).astype(jnp.bfloat16)


def plain_body(query_rows, key_rows, value_rows, out_weight):
    query_feature, key_feature = (feature_map(query_rows), feature_map(key_rows))
    count = query_rows.shape[1] * lax.axis_size("sp")
    state = (
        jnp.einsum("bthd,bthe->bhde", key_feature, value_rows, preferred_element_type=jnp.float32)
        / count
    )
    mass = jnp.sum(key_feature.astype(jnp.float32), axis=1) / count
    state = lax.psum(state.astype(jnp.bfloat16), "sp")
    mass = lax.psum(mass, "sp")
    top = jnp.einsum("bthd,bhde->bthe", query_feature, state, preferred_element_type=jnp.float32)
    bottom = jnp.einsum(
        "bthd,bhd->bth", query_feature.astype(jnp.float32), mass, precision=lax.Precision.HIGHEST
    )
    mixed = (top / (bottom + 0.001)[..., None] * count**0.5).astype(jnp.bfloat16)
    mixed = mixed.reshape(mixed.shape[0], mixed.shape[1], -1)
    mine = lax.all_to_all(mixed, "dp", split_axis=2, concat_axis=0, tiled=True)
    part = jnp.einsum("btw,wv->btv", mine, out_weight, preferred_element_type=jnp.float32)
    return lax.psum_scatter(part.astype(jnp.bfloat16), "dp", scatter_dimension=0, tiled=True)


MESH = pl.DeviceIdType.MESH
NT = (((1,), (1,)), ((), ()))
TN = (((0,), (0,)), ((), ()))
EXTRA = 16
PART = 2


def feature32(values):
    wide = values.astype(jnp.float32)
    return jnp.where(wide > 0.0, wide + 1.0, jnp.exp(jnp.minimum(wide, 0.0)))


def remote(src, dst, send, recv, **where):
    return pltpu.make_async_remote_copy(
        src_ref=src, dst_ref=dst, send_sem=send, recv_sem=recv, device_id=where, device_id_type=MESH
    )


def kernel(
    NS, count, q_hbm, k_hbm, v_hbm, w_hbm, out_hbm,
    kin, vin, qin, wide, wide2, w, own, up, inb, cb, sall, qf, mixed,
    m1, r1, s2, r2, keep,
    ksem, vsem, lsem, wsem, qs, qr, us, inr, cbr, ds, sts, fws, str_, s1, t1, s2s, s2r,
):
    d, p = lax.axis_index("dp"), lax.axis_index("sp")
    i, j = lax.div(d, 2), lax.rem(d, 2)
    T, HD, size = kin.shape[1:]
    G, SUB = up.shape[0], sall.shape[1]
    C = keep.shape[-1]
    NC = w.shape[1] // C
    mid, HALF, EVEN = NS // 2, SUB // 2, m1.shape[1]
    ODD = NC - EVEN

    def peer(r):
        return lax.rem(i + r // 2, 2) * 2 + lax.rem(j + r % 2, 2)

    left = p < mid
    side = 1 - lax.div(p, mid)
    center = p - 1 + 2 * side
    outer = p + 1 - 2 * side
    is_mid = jnp.logical_or(p == mid - 1, p == mid)
    has_outer = jnp.logical_and(p > 0, p < NS - 1)
    has_inner = jnp.logical_not(is_mid)

    loads = {}
    for n in range(4):
        rows = pl.ds(peer((n + 1) % 4) * HD, HD)
        loads[n] = (
            pltpu.make_async_copy(k_hbm.at[:, rows], kin.at[n], ksem.at[n]),
            pltpu.make_async_copy(v_hbm.at[:, rows], vin.at[n], vsem.at[n]),
        )
        loads[n][0].start()
        loads[n][1].start()

    barrier = pltpu.get_barrier_semaphore()
    for r in (1, 2, 3):
        pl.semaphore_signal(barrier, inc=1, device_id={"dp": peer(r)}, device_id_type=MESH)
    pl.semaphore_signal(barrier, inc=1, device_id={"sp": center}, device_id_type=MESH)

    @pl.when(has_outer)
    def _():
        pl.semaphore_signal(barrier, inc=1, device_id={"sp": outer}, device_id_type=MESH)
        pl.semaphore_wait(barrier, 5)

    @pl.when(jnp.logical_not(has_outer))
    def _():
        pl.semaphore_wait(barrier, 4)

    PIECES = 4
    queries = []
    for r in (1, 2, 3):
        pieces = PIECES if r == 3 else 1
        for x in range(pieces):
            tokens = pl.ds(x * (T // pieces), T // pieces)
            source = q_hbm.at[tokens, pl.ds(peer(r) * HD, HD)]
            n = r - 1 + x
            queries.append(remote(source, qin.at[r, tokens], qs.at[n], qr.at[n], dp=peer(r)))
    queries[0].start()
    queries[1].start()
    own_query = pltpu.make_async_copy(q_hbm.at[:, pl.ds(d * HD, HD)], qin.at[0], lsem)
    weights = pltpu.make_async_copy(w_hbm, w, wsem)

    def widen(src, dst, fn):
        step = 64

        @pl.loop(0, T // step)
        def _(x):
            block = fn(src[pl.ds(pl.multiple_of(x * step, step), step)])
            rows = step * HD
            dst[pl.ds(pl.multiple_of(x * rows, rows), rows)] = block.reshape(rows, size)

    def up_end(g):
        return remote(up.at[g], inb.at[g], us.at[g], inr.at[g], sp=center)

    def up_mid(g):
        return remote(up.at[g], cb.at[g], us.at[g], cbr.at[g], sp=center)

    def down(g):
        return remote(cb.at[g], cb.at[g], ds.at[g], cbr.at[g], sp=outer)

    def spread(n, x):
        return remote(
            cb.at[n * SUB + x], sall.at[n, x], sts.at[n, lax.rem(x, HALF)], str_.at[n, x], dp=peer((n + 1) % 4)
        )

    def forward(n, x, to):
        return remote(sall.at[n, x], sall.at[n, x], fws.at[n, lax.rem(x, HALF)], str_.at[n, x], sp=to)

    for n in range(4):
        loads[n][0].wait()
        loads[n][1].wait()
        widen(kin.at[n], wide, feature32)
        widen(vin.at[n], wide2, lambda x: x.astype(jnp.float32))

        @pl.loop(0, SUB)
        def _(x):
            g = n * SUB + x
            row = lax.broadcasted_iota(jnp.int32, (EXTRA, size), 0)
            masses = jnp.zeros((EXTRA, size), jnp.float32)
            for k in range(PART):
                key = wide[pl.ds(x * PART + k, T, stride=HD), :].astype(jnp.bfloat16)
                value = wide2[pl.ds(x * PART + k, T, stride=HD), :].astype(jnp.bfloat16)
                state = lax.dot_general(value, key, TN, preferred_element_type=jnp.float32) / count
                mass = jnp.sum(key.astype(jnp.float32), axis=0, keepdims=True) / count
                masses = jnp.where(row == k, mass, masses)
                own[g, k * size : (k + 1) * size] = state
                up[g, k * size : (k + 1) * size] = state.astype(up.dtype)
            own[g, PART * size :] = masses
            up[g, PART * size :] = masses.astype(up.dtype)

            if n < 3:

                @pl.when(has_inner)
                def _():
                    up_end(g).start()

    own_query.start()
    weights.start()

    def take_in(g):
        up_end(g).wait_recv()
        total = own[g] + inb[g].astype(jnp.float32)
        own[g] = total
        up[g] = total.astype(up.dtype)
        up_mid(g).start()

    LAG = 2

    def reduce_states(n, begin=0, end=None):
        end = SUB if end is None else end

        @pl.when(is_mid)
        def _():
            if n % 3 == 0 and begin == 0:
                for x in range(LAG):
                    take_in(n * SUB + x)

            @pl.loop(begin, end)
            def _(x):
                g = n * SUB + x

                @pl.when(x + LAG < (SUB if n > 1 else G))
                def _():
                    take_in(g + LAG)

                up_mid(g).wait_recv()
                cb[g] = (own[g] + cb[g].astype(jnp.float32)).astype(cb.dtype)

                if n == 3:
                    down(g).start()
                else:

                    @pl.when(x < HALF)
                    def _():
                        down(g).start()

                    @pl.when(x >= HALF)
                    def _():
                        spread(n, x).start()

        @pl.when(has_inner)
        def _():
            @pl.loop(begin, end if n == 3 else max(begin, min(end, HALF)))
            def _(x):
                up_mid(n * SUB + x).wait_recv()
                if n < 3:
                    spread(n, x).start()

    def exchange(n):
        for role, begin, to in ((has_inner, 0, center), (is_mid, HALF, outer)):

            @pl.when(role)
            def _():
                for x in range(begin, begin + HALF):
                    forward(n, x, to).wait_recv()
                    forward(n, x, to).start()

    def query_features(r):
        widen(qin.at[r], wide, feature32)
        for k in range(HD):
            qf[r, k] = wide[pl.ds(k, T, stride=HD), :].astype(qf.dtype)

    def mix(r, states):
        for k in range(HD):
            x, kk = k // PART, k % PART
            block = states(x)
            masses = block[PART * size :].astype(jnp.float32)
            mass = jnp.broadcast_to(masses[kk : kk + 1], (size, size)).astype(jnp.bfloat16)
            both = jnp.concatenate([block[kk * size : (kk + 1) * size], mass], axis=0)
            read = lax.dot_general(qf[r, k], both, NT, preferred_element_type=jnp.float32)
            read = read[:, :size] / (read[:, size:] + 0.001) * count**0.5
            mixed[r, :, k * size : (k + 1) * size] = read.astype(mixed.dtype)

    def wait_spread(n):
        for role, begin, to in ((has_inner, HALF, center), (is_mid, 0, outer)):

            @pl.when(role)
            def _():
                for x in range(begin, begin + HALF):
                    forward(n, x, to).wait_recv()

    def columns(c, odd):
        return pl.ds(pl.multiple_of((EVEN * odd + c) * C, C), C)

    def every(body):
        @pl.loop(0, ODD)
        def _(c):
            body(c, 0)
            body(c, 1)

        @pl.loop(ODD, EVEN)
        def _(c):
            body(c, 0)

    def first(c, odd, diagonal):
        return remote(
            m1.at[odd, c, diagonal], r1.at[odd, c, diagonal], s1.at[odd, c, diagonal], t1.at[odd, c, diagonal],
            dp=peer(2 if odd else 1),
        )

    def second(c, odd):
        return remote(s2.at[odd, c], r2.at[odd, c], s2s.at[odd, c], s2r.at[odd, c], dp=peer(1 if odd else 2))

    def times(r, c, odd):
        return jnp.dot(mixed[r], w[:, columns(c, odd)], preferred_element_type=jnp.float32)

    def neighbour_messages(c, odd):
        m1[odd, c, 0] = times(2 if odd else 1, c, odd).astype(m1.dtype)
        first(c, odd, 0).start()

    queries[2].start()
    reduce_states(0)
    queries[3].start()
    queries[0].wait_recv()
    query_features(1)
    reduce_states(1)
    exchange(0)
    queries[4].start()
    queries[1].wait_recv()
    query_features(2)
    reduce_states(2, 0, HALF)
    exchange(1)
    reduce_states(2, HALF)
    queries[5].start()

    @pl.when(has_inner)
    def _():
        for g in range(3 * SUB, G):
            up_end(g).start()

    weights.wait()
    wait_spread(0)
    mix(1, lambda x: sall[0, x])
    neighbour_messages(0, 0)
    wait_spread(1)
    mix(2, lambda x: sall[1, x])
    neighbour_messages(0, 1)

    @pl.loop(1, EVEN)
    def _(c):
        neighbour_messages(c, 0)

        @pl.when(c < ODD)
        def _():
            neighbour_messages(c, 1)

    exchange(2)
    for x in range(PIECES):
        queries[2 + x].wait_recv()
    query_features(3)
    wait_spread(2)
    mix(3, lambda x: sall[2, x])

    @every
    def diagonal_messages(c, odd):
        m1[odd, c, 1] = times(3, c, odd).astype(m1.dtype)
        first(c, odd, 1).start()

    reduce_states(3)
    own_query.wait()
    query_features(0)
    mix(0, lambda x: cb[3 * SUB + x])

    @every
    def own_sums(c, odd):
        block = times(0, c, odd)
        first(c, odd, 0).wait_recv()
        keep[odd, c] = block + r1[odd, c, 0].astype(jnp.float32)

    @every
    def second_messages(c, odd):
        block = times(1 if odd else 2, c, odd)
        first(c, odd, 1).wait_recv()
        s2[odd, c] = (block + r1[odd, c, 1].astype(jnp.float32)).astype(s2.dtype)
        second(c, odd).start()

    @every
    def last_sums(c, odd):
        second(c, odd).wait_recv()
        out_hbm[:, columns(c, odd)] = (keep[odd, c] + r2[odd, c].astype(jnp.float32)).astype(out_hbm.dtype)

    for query in queries:
        query.wait_send()

    @pl.loop(0, G)
    def _(g):
        up_end(g).wait_send()

    for role, begin, to in ((has_inner, 0, center), (is_mid, HALF, outer)):

        @pl.when(role)
        def _():
            for n in range(3):
                for x in range(begin, begin + HALF):
                    spread(n, x).wait_send()
                    forward(n, x, to).wait_send()

    @pl.when(has_outer)
    def _():
        for n in range(4):
            for x in range(SUB if n == 3 else HALF):
                down(n * SUB + x).wait_send()

    @every
    def drain(c, odd):
        first(c, odd, 0).wait_send()
        first(c, odd, 1).wait_send()
        second(c, odd).wait_send()


def kernel_body(query_rows, key_rows, value_rows, out_weight):
    NS = lax.axis_size("sp")
    _, T, H, size = query_rows.shape
    V, rows = out_weight.shape[1], out_weight.shape[0]
    HD, NC, EVEN = H // 4, 16, 8
    C, count = V // NC, T * NS
    SUB = HD // PART
    G, R = 4 * SUB, PART * size + EXTRA
    bf, f32 = jnp.bfloat16, jnp.float32
    dma = pltpu.SemaphoreType.DMA
    hbm = pl.BlockSpec(memory_space=pl.ANY)
    out = pl.pallas_call(
        functools.partial(kernel, NS, count),
        out_shape=jax.ShapeDtypeStruct((T, V), bf),
        in_specs=[hbm] * 4,
        out_specs=pl.BlockSpec(memory_space=pltpu.VMEM),
        scratch_shapes=[
            pltpu.VMEM((4, T, HD, size), bf),
            pltpu.VMEM((4, T, HD, size), bf),
            pltpu.VMEM((4, T, HD, size), bf),
            pltpu.VMEM((T * HD, size), f32),
            pltpu.VMEM((T * HD, size), f32),
            pltpu.VMEM((rows, V), bf),
            pltpu.VMEM((G, R, size), f32),
            pltpu.VMEM((G, R, size), bf),
            pltpu.VMEM((G, R, size), bf),
            pltpu.VMEM((G, R, size), bf),
            pltpu.VMEM((3, SUB, R, size), bf),
            pltpu.VMEM((4, HD, T, size), bf),
            pltpu.VMEM((4, T, rows), bf),
            pltpu.VMEM((2, EVEN, 2, T, C), bf),
            pltpu.VMEM((2, EVEN, 2, T, C), bf),
            pltpu.VMEM((2, EVEN, T, C), bf),
            pltpu.VMEM((2, EVEN, T, C), bf),
            pltpu.VMEM((2, EVEN, T, C), f32),
            dma((4,)), dma((4,)), dma, dma, dma((6,)), dma((6,)),
            dma((G,)), dma((G,)), dma((G,)), dma((G,)), dma((3, SUB // 2)), dma((3, SUB // 2)), dma((3, SUB)),
            dma((2, EVEN, 2)), dma((2, EVEN, 2)), dma((2, EVEN)), dma((2, EVEN)),
        ],
        compiler_params=pltpu.CompilerParams(
            collective_id=0, has_side_effects=True, vmem_limit_bytes=50 * 2**20
        ),
    )(query_rows[0], key_rows[0], value_rows[0], out_weight)
    return out[None]


def split_of(n):
    for a in range(int(n**0.5), 0, -1):
        if n % a == 0:
            return a, n // a


def body(query_rows, key_rows, value_rows, out_weight):
    ND, NS = lax.axis_size("dp"), lax.axis_size("sp")
    batch, T, H, size = query_rows.shape
    rows, V = out_weight.shape
    fits = batch == 1 and split_of(ND) == (2, 2) and NS == 4 and H % 4 == 0 and (H // 4) % 8 == 0
    fits = fits and size == 128 and T % 64 == 0 and V % 4096 == 0 and rows * 4 == H * size
    need = 2 * rows * V + 18 * T * V + 12 * T * H * size + 14 * H * size * size
    run = kernel_body if fits and need < 50 * 2**20 else plain_body
    return run(query_rows, key_rows, value_rows, out_weight)


def solution(mesh):
    placed = (
        P(("shift", "dp"), "sp", None, None),
        P(("shift", "dp"), "sp", None, None),
        P(("shift", "dp"), "sp", None, None),
        P(("shift", "dp"), None),
    )
    return jax.shard_map(
        body, mesh=mesh, in_specs=placed, out_specs=P(("shift", "dp"), "sp", None), check_vma=False
    )
```

```python
import functools

import jax
import jax.numpy as jnp
from jax import lax
from jax.experimental import pallas as pl
from jax.experimental.pallas import tpu as pltpu
from jax.sharding import PartitionSpec as P


def feature_map(values):
    wide = values.astype(jnp.float32)
    return jnp.where(wide > 0.0, wide + 1.0, jnp.exp(jnp.minimum(wide, 0.0))).astype(jnp.bfloat16)


def plain_body(query_rows, key_rows, value_rows, out_weight):
    query_feature, key_feature = (feature_map(query_rows), feature_map(key_rows))
    count = query_rows.shape[1] * lax.axis_size("sp")
    state = (
        jnp.einsum("bthd,bthe->bhde", key_feature, value_rows, preferred_element_type=jnp.float32)
        / count
    )
    mass = jnp.sum(key_feature.astype(jnp.float32), axis=1) / count
    state = lax.psum(state.astype(jnp.bfloat16), "sp")
    mass = lax.psum(mass, "sp")
    top = jnp.einsum("bthd,bhde->bthe", query_feature, state, preferred_element_type=jnp.float32)
    bottom = jnp.einsum(
        "bthd,bhd->bth", query_feature.astype(jnp.float32), mass, precision=lax.Precision.HIGHEST
    )
    mixed = (top / (bottom + 0.001)[..., None] * count**0.5).astype(jnp.bfloat16)
    mixed = mixed.reshape(mixed.shape[0], mixed.shape[1], -1)
    mine = lax.all_to_all(mixed, "dp", split_axis=2, concat_axis=0, tiled=True)
    part = jnp.einsum("btw,wv->btv", mine, out_weight, preferred_element_type=jnp.float32)
    return lax.psum_scatter(part.astype(jnp.bfloat16), "dp", scatter_dimension=0, tiled=True)


MESH = pl.DeviceIdType.MESH
NT = (((1,), (1,)), ((), ()))
TN = (((0,), (0,)), ((), ()))
EXTRA = 16
PART = 2


def feature32(values):
    wide = values.astype(jnp.float32)
    return jnp.where(wide > 0.0, wide + 1.0, jnp.exp(jnp.minimum(wide, 0.0)))


def remote(src, dst, send, recv, **where):
    return pltpu.make_async_remote_copy(
        src_ref=src, dst_ref=dst, send_sem=send, recv_sem=recv, device_id=where, device_id_type=MESH
    )


def kernel(
    NS, count, q_hbm, k_hbm, v_hbm, w_hbm, out_ref,
    kv, qin, wide, wide2, w, own, up, inb, cb, sall, qf, mixed,
    m1, r1, s2, r2, keep,
    ksem, lsem, wsem, qs, qr, us, inr, cbr, ds, sts, fws, str_, s1, t1, s2s, s2r,
):
    d, p = lax.axis_index("dp"), lax.axis_index("sp")
    i, j = lax.div(d, 2), lax.rem(d, 2)
    T, HD, size = qin.shape[1:]
    G, SUB = up.shape[0], sall.shape[1]
    C = keep.shape[-1]
    NC = w.shape[1] // C
    mid, half = NS // 2, NC // 2

    def peer(r):
        return lax.rem(i + r // 2, 2) * 2 + lax.rem(j + r % 2, 2)

    side = 1 - lax.div(p, mid)
    center = p - 1 + 2 * side
    outer = p + 1 - 2 * side
    is_mid = jnp.logical_or(p == mid - 1, p == mid)
    has_outer = jnp.logical_and(p > 0, p < NS - 1)
    has_inner = jnp.logical_not(is_mid)
    inside = lax.div(lax.rem(p, NS - 1) + 1, 2)
    mine = inside * (p + 1) + (1 - inside) * lax.div(p, NS - 1)

    for n in range(4):
        rows = pl.ds(peer((n + 1) % 4) * HD, HD)
        pltpu.make_async_copy(k_hbm.at[:, rows], kv.at[n, 0], ksem.at[n]).start()
        pltpu.make_async_copy(v_hbm.at[:, rows], kv.at[n, 1], ksem.at[n]).start()

    barrier = pltpu.get_barrier_semaphore()
    for r in (1, 2, 3):
        pl.semaphore_signal(barrier, inc=1, device_id={"dp": peer(r)}, device_id_type=MESH)
    for x in range(1, NS):
        pl.semaphore_signal(barrier, inc=1, device_id={"sp": lax.rem(p + x, NS)}, device_id_type=MESH)
    pl.semaphore_wait(barrier, 2 + NS)

    PIECES, FIRST, DELAY = 8, 3, 1
    def piece(k):
        tokens = pl.ds(pl.multiple_of(k * (T // PIECES), T // PIECES), T // PIECES)
        source = q_hbm.at[tokens, pl.ds(peer(3) * HD, HD)]
        return remote(source, qin.at[3, tokens], qs, qr.at[2], dp=peer(3))

    queries = {}
    for r in (1, 2):
        source = q_hbm.at[:, pl.ds(peer(r) * HD, HD)]
        queries[r] = remote(source, qin.at[r], qs, qr.at[r - 1], dp=peer(r))
        queries[r].start()
    own_query = pltpu.make_async_copy(q_hbm.at[:, pl.ds(d * HD, HD)], qin.at[0], lsem)
    for k in range(FIRST):
        piece(k).start()
    weights = pltpu.make_async_copy(w_hbm, w, wsem)

    def widen(src, dst, fn):
        step = 64

        @pl.loop(0, T // step)
        def _(x):
            block = fn(src[pl.ds(pl.multiple_of(x * step, step), step)])
            rows = step * HD
            dst[pl.ds(pl.multiple_of(x * rows, rows), rows)] = block.reshape(rows, size)

    def place(k):
        return (k % 2) * SUB + k // 2

    def up_end(g):
        return remote(up.at[g], inb.at[g], us, inr.at[g], sp=center)

    def up_mid(g):
        return remote(up.at[g], cb.at[g], us, cbr.at[g], sp=center)

    def down(g):
        return remote(cb.at[g], cb.at[g], ds, cbr.at[g], sp=outer)

    def spread(n, x):
        r = n + 1
        dd = (i + r // 2) % 2 * 2 + (j + r) % 2
        return remote(cb.at[n * SUB + x], sall.at[n, x], sts, str_.at[n, x], dp=dd)

    def forward(x):
        return remote(sall.at[2, mine], sall.at[2, mine], fws, str_.at[2, mine], sp=lax.rem(p + x, NS))

    for n in range(4):
        pltpu.make_async_copy(kv.at[n], kv.at[n], ksem.at[n]).wait()
        widen(kv.at[n, 0], wide, feature32)
        widen(kv.at[n, 1], wide2, lambda x: x.astype(jnp.float32))

        @pl.loop(0, SUB)
        def _(x):
            g = n * SUB + x
            row = lax.broadcasted_iota(jnp.int32, (EXTRA, size), 0)
            masses = jnp.zeros((EXTRA, size), jnp.float32)
            for k in range(PART):
                key = wide[pl.ds(x * PART + k, T, stride=HD), :].astype(jnp.bfloat16)
                value = wide2[pl.ds(x * PART + k, T, stride=HD), :].astype(jnp.bfloat16)
                state = lax.dot_general(value, key, TN, preferred_element_type=jnp.float32) / count
                mass = jnp.sum(key.astype(jnp.float32), axis=0, keepdims=True) / count
                masses = jnp.where(row == k, mass, masses)
                own[g, k * size : (k + 1) * size] = state
                up[g, k * size : (k + 1) * size] = state.astype(up.dtype)
            own[g, PART * size :] = masses
            up[g, PART * size :] = masses.astype(up.dtype)

        @pl.when(has_inner)
        def _():
            if n == 0:
                up_end(0).start()
            if n == 1:
                for k in range(1, 2 * SUB):
                    up_end(place(k)).start()
            if n == 2:
                for g in range(2 * SUB, 3 * SUB):
                    up_end(g).start()

    own_query.start()
    weights.start()

    def take_in(g, both):
        up_end(g).wait_recv()
        total = own[g] + inb[g].astype(jnp.float32)
        keeps = lax.rem(g, 2) == p - 1

        def hold():
            own[g] = total

        def send():
            up[g] = total.astype(up.dtype)
            up_mid(g).start()

        if both:
            hold()
            send()
        else:
            pl.when(keeps)(hold)
            pl.when(jnp.logical_not(keeps))(send)

    def finish(g):
        up_mid(g).wait_recv()
        cb[g] = (own[g] + cb[g].astype(jnp.float32)).astype(cb.dtype)

    LAG = 2

    def reduce_neighbours():
        def step(k):
            n, x = k % 2, k // 2
            spread(n, x).start()

            @pl.when(k >= FIRST + DELAY)
            def _():
                piece(k - DELAY).start()

        @pl.when(is_mid)
        def _():
            for k in range(LAG):
                take_in(place(k), True)

            @pl.loop(0, 2 * SUB)
            def _(k):
                @pl.when(k + LAG < 2 * SUB)
                def _():
                    take_in(place(k + LAG), True)

                finish(place(k))
                down(place(k)).start()
                step(k)

        @pl.when(has_inner)
        def _():
            @pl.loop(0, 2 * SUB)
            def _(k):
                up_mid(place(k)).wait_recv()
                step(k)

    def reduce_diagonal():
        @pl.when(is_mid)
        def _():
            @pl.loop(2 * SUB, 3 * SUB)
            def _(g):
                take_in(g, False)

            for x in range(2):
                g = 2 * SUB + 2 * x + p - 1
                finish(g)
                if x == 0:
                    down(g).start()

        @pl.when(has_inner)
        def _():
            up_mid(2 * SUB + mine).wait_recv()

        spread(2, mine).start()

    def reduce_own():
        @pl.when(is_mid)
        def _():
            @pl.loop(3 * SUB, G)
            def _(g):
                take_in(g, True)

            @pl.loop(3 * SUB, G)
            def _(g):
                finish(g)
                down(g).start()

        @pl.when(has_inner)
        def _():
            @pl.loop(3 * SUB, G)
            def _(g):
                up_mid(g).wait_recv()

    def exchange():
        forward(1).wait_recv()
        for x in range(1, NS):
            forward(x).start()

    def query_features(r):
        widen(qin.at[r], wide, feature32)
        for k in range(HD):
            qf[r, k] = wide[pl.ds(k, T, stride=HD), :].astype(qf.dtype)

    def mix(r, states):
        for k in range(HD):
            x, kk = k // PART, k % PART
            block = states(x)
            masses = block[PART * size :].astype(jnp.float32)
            mass = jnp.broadcast_to(masses[kk : kk + 1], (size, size)).astype(jnp.bfloat16)
            both = jnp.concatenate([block[kk * size : (kk + 1) * size], mass], axis=0)
            read = lax.dot_general(qf[r, k], both, NT, preferred_element_type=jnp.float32)
            read = read[:, :size] / (read[:, size:] + 0.001) * count**0.5
            mixed[r, :, k * size : (k + 1) * size] = read.astype(mixed.dtype)

    def wait_spread(n):
        for x in range(SUB):

            def wait():
                spread(n, x).wait_recv()

            if n < 2:
                wait()
            else:
                pl.when(x != mine)(wait)

    def columns(c, odd):
        return pl.ds(pl.multiple_of((2 * c + odd) * C, C), C)

    def first(c, odd, diagonal):
        recv = t1.at[2 + c] if diagonal else t1.at[odd]
        return remote(
            m1.at[diagonal, c, odd], r1.at[diagonal, c, odd], s1, recv, dp=peer(2 if odd else 1)
        )

    def second(c, odd):
        return remote(s2.at[c, odd], r2.at[c, odd], s2s, s2r.at[c], dp=peer(1 if odd else 2))

    def arrived(ref, semaphore):
        pltpu.make_async_copy(ref, ref, semaphore).wait()

    def times(r, c, odd):
        return jnp.dot(mixed[r], w[:, columns(c, odd)], preferred_element_type=jnp.float32)

    def neighbour_messages(c, odd):
        m1[0, c, odd] = times(2 if odd else 1, c, odd).astype(m1.dtype)
        first(c, odd, 0).start()

    reduce_neighbours()
    for k in range(2 * SUB - DELAY, PIECES):
        piece(k).start()
    for r in (1, 2):
        queries[r].wait_recv()
        query_features(r)
    reduce_diagonal()
    weights.wait()
    wait_spread(0)
    mix(1, lambda x: sall[0, x])
    neighbour_messages(0, 0)
    wait_spread(1)
    mix(2, lambda x: sall[1, x])
    neighbour_messages(0, 1)

    @pl.when(has_inner)
    def _():
        for g in range(3 * SUB, G):
            up_end(g).start()

    @pl.loop(1, half)
    def _(c):
        for odd in range(2):
            neighbour_messages(c, odd)

    exchange()
    arrived(qin.at[3], qr.at[2])
    query_features(3)
    wait_spread(2)
    mix(3, lambda x: sall[2, x])

    @pl.loop(0, half)
    def _(c):
        for odd in range(2):
            m1[1, c, odd] = times(3, c, odd).astype(m1.dtype)
            first(c, odd, 1).start()

    reduce_own()
    own_query.wait()
    query_features(0)
    mix(0, lambda x: cb[3 * SUB + x])

    for odd in range(2):
        arrived(s2.at[:, odd], t1.at[odd])

    @pl.loop(0, half)
    def _(c):
        for odd in range(2):
            keep[c, odd] = times(0, c, odd) + r1[0, c, odd].astype(jnp.float32)

    @pl.loop(0, half)
    def _(c):
        blocks = [times(1 if odd else 2, c, odd) for odd in range(2)]
        arrived(r1.at[1, c], t1.at[2 + c])
        for odd in range(2):
            s2[c, odd] = (blocks[odd] + r1[1, c, odd].astype(jnp.float32)).astype(s2.dtype)
            second(c, odd).start()

    @pl.loop(0, half)
    def _(c):
        arrived(r2.at[c], s2r.at[c])
        for odd in range(2):
            total = keep[c, odd] + r2[c, odd].astype(jnp.float32)
            out_ref[:, columns(c, odd)] = total.astype(out_ref.dtype)

    arrived(qin.at[pl.ds(0, 3)], qs)
    arrived(up.at[pl.ds(0, 2 * SUB + 1)], sts)
    arrived(up.at[pl.ds(0, NS - 1)], fws)
    arrived(m1, s1)
    arrived(s2, s2s)

    @pl.when(has_inner)
    def _():
        arrived(up, us)

    @pl.when(is_mid)
    def _():
        arrived(up.at[pl.ds(0, 3 * SUB + 2)], us)
        arrived(up.at[pl.ds(0, 3 * SUB + 1)], ds)


def kernel_body(query_rows, key_rows, value_rows, out_weight):
    NS = lax.axis_size("sp")
    _, T, H, size = query_rows.shape
    V, rows = out_weight.shape[1], out_weight.shape[0]
    HD, NC = H // 4, 16
    C, half, count = V // NC, NC // 2, T * NS
    SUB = HD // PART
    G, R = 4 * SUB, PART * size + EXTRA
    bf, f32 = jnp.bfloat16, jnp.float32
    dma = pltpu.SemaphoreType.DMA
    hbm = pl.BlockSpec(memory_space=pl.ANY)
    out = pl.pallas_call(
        functools.partial(kernel, NS, count),
        out_shape=jax.ShapeDtypeStruct((T, V), bf),
        in_specs=[hbm] * 4,
        out_specs=pl.BlockSpec(memory_space=pltpu.VMEM),
        scratch_shapes=[
            pltpu.VMEM((4, 2, T, HD, size), bf),
            pltpu.VMEM((4, T, HD, size), bf),
            pltpu.VMEM((T * HD, size), f32),
            pltpu.VMEM((T * HD, size), f32),
            pltpu.VMEM((rows, V), bf),
            pltpu.VMEM((G, R, size), f32),
            pltpu.VMEM((G, R, size), bf),
            pltpu.VMEM((G, R, size), bf),
            pltpu.VMEM((G, R, size), bf),
            pltpu.VMEM((3, SUB, R, size), bf),
            pltpu.VMEM((4, HD, T, size), bf),
            pltpu.VMEM((4, T, rows), bf),
            pltpu.VMEM((2, half, 2, T, C), bf),
            pltpu.VMEM((2, half, 2, T, C), bf),
            pltpu.VMEM((half, 2, T, C), bf),
            pltpu.VMEM((half, 2, T, C), bf),
            pltpu.VMEM((half, 2, T, C), f32),
            dma((4,)), dma, dma, dma, dma((3,)),
            dma, dma((G,)), dma((G,)), dma, dma, dma, dma((3, SUB)),
            dma, dma((2 + half,)), dma, dma((half,)),
        ],
        compiler_params=pltpu.CompilerParams(
            collective_id=0, has_side_effects=True, vmem_limit_bytes=50 * 2**20
        ),
    )(query_rows[0], key_rows[0], value_rows[0], out_weight)
    return out[None]


def split_of(n):
    for a in range(int(n**0.5), 0, -1):
        if n % a == 0:
            return a, n // a


def body(query_rows, key_rows, value_rows, out_weight):
    ND, NS = lax.axis_size("dp"), lax.axis_size("sp")
    batch, T, H, size = query_rows.shape
    rows, V = out_weight.shape
    fits = batch == 1 and split_of(ND) == (2, 2) and NS == 4 and H // 4 == 4 * PART
    fits = fits and size == 128 and T % 64 == 0 and V % 4096 == 0 and rows * 4 == H * size
    need = 2 * rows * V + 18 * T * V + 12 * T * H * size + 14 * H * size * size
    run = kernel_body if fits and need < 50 * 2**20 else plain_body
    return run(query_rows, key_rows, value_rows, out_weight)


def solution(mesh):
    placed = (
        P(("shift", "dp"), "sp", None, None),
        P(("shift", "dp"), "sp", None, None),
        P(("shift", "dp"), "sp", None, None),
        P(("shift", "dp"), None),
    )
    return jax.shard_map(
        body, mesh=mesh, in_specs=placed, out_specs=P(("shift", "dp"), "sp", None), check_vma=False
    )
```

```python
import functools

import jax
import jax.numpy as jnp
from jax import lax
from jax.experimental import pallas as pl
from jax.experimental.pallas import tpu as pltpu
from jax.sharding import PartitionSpec as P


def feature_map(values):
    wide = values.astype(jnp.float32)
    return jnp.where(wide > 0.0, wide + 1.0, jnp.exp(jnp.minimum(wide, 0.0))).astype(jnp.bfloat16)


def plain_body(query_rows, key_rows, value_rows, out_weight):
    query_feature, key_feature = (feature_map(query_rows), feature_map(key_rows))
    count = query_rows.shape[1] * lax.axis_size("sp")
    state = (
        jnp.einsum("bthd,bthe->bhde", key_feature, value_rows, preferred_element_type=jnp.float32)
        / count
    )
    mass = jnp.sum(key_feature.astype(jnp.float32), axis=1) / count
    state = lax.psum(state.astype(jnp.bfloat16), "sp")
    mass = lax.psum(mass, "sp")
    top = jnp.einsum("bthd,bhde->bthe", query_feature, state, preferred_element_type=jnp.float32)
    bottom = jnp.einsum(
        "bthd,bhd->bth", query_feature.astype(jnp.float32), mass, precision=lax.Precision.HIGHEST
    )
    mixed = (top / (bottom + 0.001)[..., None] * count**0.5).astype(jnp.bfloat16)
    mixed = mixed.reshape(mixed.shape[0], mixed.shape[1], -1)
    mine = lax.all_to_all(mixed, "dp", split_axis=2, concat_axis=0, tiled=True)
    part = jnp.einsum("btw,wv->btv", mine, out_weight, preferred_element_type=jnp.float32)
    return lax.psum_scatter(part.astype(jnp.bfloat16), "dp", scatter_dimension=0, tiled=True)


MESH = pl.DeviceIdType.MESH
NT = (((1,), (1,)), ((), ()))
TN = (((0,), (0,)), ((), ()))
EXTRA = 16
PART = 2


def feature32(values):
    wide = values.astype(jnp.float32)
    return jnp.where(wide > 0.0, wide + 1.0, jnp.exp(jnp.minimum(wide, 0.0)))


def remote(src, dst, send, recv, **where):
    return pltpu.make_async_remote_copy(
        src_ref=src, dst_ref=dst, send_sem=send, recv_sem=recv, device_id=where, device_id_type=MESH
    )


def kernel(
    NS, count, q_hbm, k_hbm, v_hbm, w_hbm, out_ref,
    kv, qin, wide, wide2, w, own, up, inb, cb, sall, qf, mixed,
    m1, r1, s2, r2, keep,
    ksem, lsem, wsem, qs, qr, us, inr, cbr, ds, sts, fws, str_, s1, t1, s2s, s2r,
):
    d, p = lax.axis_index("dp"), lax.axis_index("sp")
    i, j = lax.div(d, 2), lax.rem(d, 2)
    T, HD, size = qin.shape[1:]
    G, SUB = up.shape[0], sall.shape[1]
    C = keep.shape[-1]
    NC = w.shape[1] // C
    mid, half = NS // 2, NC // 2

    def peer(r):
        return lax.rem(i + r // 2, 2) * 2 + lax.rem(j + r % 2, 2)

    side = 1 - lax.div(p, mid)
    center = p - 1 + 2 * side
    outer = p + 1 - 2 * side
    is_mid = jnp.logical_or(p == mid - 1, p == mid)
    has_outer = jnp.logical_and(p > 0, p < NS - 1)
    has_inner = jnp.logical_not(is_mid)
    inside = lax.div(lax.rem(p, NS - 1) + 1, 2)
    mine = inside * (p + 1) + (1 - inside) * lax.div(p, NS - 1)

    for n in range(4):
        rows = pl.ds(peer((n + 1) % 4) * HD, HD)
        pltpu.make_async_copy(k_hbm.at[:, rows], kv.at[n, 0], ksem.at[n]).start()
        pltpu.make_async_copy(v_hbm.at[:, rows], kv.at[n, 1], ksem.at[n]).start()

    barrier = pltpu.get_barrier_semaphore()
    for r in (1, 2, 3):
        pl.semaphore_signal(barrier, inc=1, device_id={"dp": peer(r)}, device_id_type=MESH)
    for x in range(1, NS):
        pl.semaphore_signal(barrier, inc=1, device_id={"sp": lax.rem(p + x, NS)}, device_id_type=MESH)
    PIECES, FIRST = 8, 3

    def piece(k):
        tokens = pl.ds(pl.multiple_of(k * (T // PIECES), T // PIECES), T // PIECES)
        source = q_hbm.at[tokens, pl.ds(peer(3) * HD, HD)]
        return remote(source, qin.at[3, tokens], qs, qr.at[2], dp=peer(3))

    queries = {}
    for r in (1, 2):
        source = q_hbm.at[:, pl.ds(peer(r) * HD, HD)]
        queries[r] = remote(source, qin.at[r], qs, qr.at[r - 1], dp=peer(r))
    own_query = pltpu.make_async_copy(q_hbm.at[:, pl.ds(d * HD, HD)], qin.at[0], lsem)
    weights = pltpu.make_async_copy(w_hbm, w, wsem)

    def widen(src, dst, fn):
        step = 64

        @pl.loop(0, T // step)
        def _(x):
            block = fn(src[pl.ds(pl.multiple_of(x * step, step), step)])
            rows = step * HD
            dst[pl.ds(pl.multiple_of(x * rows, rows), rows)] = block.reshape(rows, size)

    def place(k):
        return (k % 2) * SUB + k // 2

    def up_end(g):
        return remote(up.at[g], inb.at[g], us, inr.at[g], sp=center)

    def up_mid(g):
        return remote(up.at[g], cb.at[g], us, cbr.at[g], sp=center)

    def down(g):
        return remote(cb.at[g], cb.at[g], ds, cbr.at[g], sp=outer)

    def spread(n, x):
        r = n + 1
        dd = (i + r // 2) % 2 * 2 + (j + r) % 2
        return remote(cb.at[n * SUB + x], sall.at[n, x], sts, str_.at[n, x], dp=dd)

    def relay(n, x, to):
        return remote(sall.at[n, x], sall.at[n, x], fws, str_.at[n, x], sp=to)

    def forward(x):
        return remote(sall.at[2, mine], sall.at[2, mine], fws, str_.at[2, mine], sp=lax.rem(p + x, NS))

    for n in range(4):
        pltpu.make_async_copy(kv.at[n], kv.at[n], ksem.at[n]).wait()
        widen(kv.at[n, 0], wide, feature32)
        widen(kv.at[n, 1], wide2, lambda x: x.astype(jnp.float32))

        if n == 0:
            pl.semaphore_wait(barrier, 2 + NS)
            for r in (1, 2):
                queries[r].start()
            for k in range(FIRST):
                piece(k).start()

        @pl.loop(0, SUB)
        def _(x):
            g = n * SUB + x
            row = lax.broadcasted_iota(jnp.int32, (EXTRA, size), 0)
            masses = jnp.zeros((EXTRA, size), jnp.float32)
            for k in range(PART):
                key = wide[pl.ds(x * PART + k, T, stride=HD), :].astype(jnp.bfloat16)
                value = wide2[pl.ds(x * PART + k, T, stride=HD), :].astype(jnp.bfloat16)
                state = lax.dot_general(value, key, TN, preferred_element_type=jnp.float32) / count
                mass = jnp.sum(key.astype(jnp.float32), axis=0, keepdims=True) / count
                masses = jnp.where(row == k, mass, masses)
                own[g, k * size : (k + 1) * size] = state
                up[g, k * size : (k + 1) * size] = state.astype(up.dtype)
            own[g, PART * size :] = masses
            up[g, PART * size :] = masses.astype(up.dtype)

        @pl.when(has_inner)
        def _():
            if n == 0:
                up_end(0).start()
            if n == 1:
                for k in range(1, 2 * SUB):
                    up_end(place(k)).start()
    own_query.start()
    weights.start()

    def take_in(g, both):
        up_end(g).wait_recv()
        total = own[g] + inb[g].astype(jnp.float32)
        keeps = lax.rem(g, 2) == p - 1

        def hold():
            own[g] = total

        def send():
            up[g] = total.astype(up.dtype)
            up_mid(g).start()

        if both:
            hold()
            send()
        else:
            pl.when(keeps)(hold)
            pl.when(jnp.logical_not(keeps))(send)

    def finish(g):
        up_mid(g).wait_recv()
        cb[g] = (own[g] + cb[g].astype(jnp.float32)).astype(cb.dtype)

    LAG = 2

    def reduce_neighbours():
        def step(t, k):
            spread(k % 2, k // 2).start()
            piece(FIRST + t).start()

        @pl.when(is_mid)
        def _():
            for k in range(LAG):
                take_in(place(k), True)

            @pl.loop(0, 2 * SUB)
            def _(k):
                @pl.when(k + LAG < 2 * SUB)
                def _():
                    take_in(place(k + LAG), True)

                finish(place(k))

                @pl.when(k < SUB)
                def _():
                    down(place(k)).start()

                @pl.when(k >= SUB)
                def _():
                    step(k - SUB, k)

        @pl.when(has_inner)
        def _():
            @pl.loop(0, SUB)
            def _(k):
                up_mid(place(k)).wait_recv()
                step(k, k)

    def swap_halves():
        for role, begin, to in ((has_inner, 0, center), (is_mid, SUB, outer)):

            @pl.when(role)
            def _():
                @pl.loop(begin, begin + SUB)
                def _(k):
                    relay(k % 2, k // 2, to).wait_recv()
                    relay(k % 2, k // 2, to).start()

    def take_diagonal():
        @pl.when(is_mid)
        def _():
            @pl.loop(2 * SUB, 3 * SUB)
            def _(g):
                take_in(g, False)

    def reduce_diagonal():
        @pl.when(is_mid)
        def _():
            for x in range(2):
                g = 2 * SUB + 2 * x + p - 1
                finish(g)
                if x == 0:
                    down(g).start()

        @pl.when(has_inner)
        def _():
            up_mid(2 * SUB + mine).wait_recv()

        spread(2, mine).start()

    def send_states(n):
        @pl.when(has_inner)
        def _():
            for g in range(n * SUB, n * SUB + SUB):
                up_end(g).start()

    def reduce_own():
        @pl.when(is_mid)
        def _():
            @pl.loop(3 * SUB, G)
            def _(g):
                take_in(g, True)

            @pl.loop(3 * SUB, G)
            def _(g):
                finish(g)
                down(g).start()

        @pl.when(has_inner)
        def _():
            @pl.loop(3 * SUB, G)
            def _(g):
                up_mid(g).wait_recv()

    def exchange():
        forward(1).wait_recv()
        for x in range(1, NS):
            forward(x).start()

    def query_features(r):
        widen(qin.at[r], wide, feature32)
        for k in range(HD):
            qf[r, k] = wide[pl.ds(k, T, stride=HD), :].astype(qf.dtype)

    def mix(r, states):
        for k in range(HD):
            x, kk = k // PART, k % PART
            block = states(x)
            masses = block[PART * size :].astype(jnp.float32)
            mass = jnp.broadcast_to(masses[kk : kk + 1], (size, size)).astype(jnp.bfloat16)
            both = jnp.concatenate([block[kk * size : (kk + 1) * size], mass], axis=0)
            read = lax.dot_general(qf[r, k], both, NT, preferred_element_type=jnp.float32)
            read = read[:, :size] / (read[:, size:] + 0.001) * count**0.5
            mixed[r, :, k * size : (k + 1) * size] = read.astype(mixed.dtype)

    def wait_spread(n):
        for x in range(SUB):
            if n < 2:
                away = is_mid if x < 2 else has_inner
            else:
                away = x != mine

            @pl.when(away)
            def _():
                spread(n, x).wait_recv()

    def columns(c, odd):
        return pl.ds(pl.multiple_of((2 * c + odd) * C, C), C)

    def first(c, odd, diagonal):
        recv = t1.at[2 + c] if diagonal else t1.at[odd]
        return remote(
            m1.at[diagonal, c, odd], r1.at[diagonal, c, odd], s1, recv, dp=peer(2 if odd else 1)
        )

    def second(c, odd):
        return remote(s2.at[c, odd], r2.at[c, odd], s2s, s2r.at[c], dp=peer(1 if odd else 2))

    def arrived(ref, semaphore):
        pltpu.make_async_copy(ref, ref, semaphore).wait()

    def times(r, c, odd):
        return jnp.dot(mixed[r], w[:, columns(c, odd)], preferred_element_type=jnp.float32)

    def neighbour_messages(c, odd):
        m1[0, c, odd] = times(2 if odd else 1, c, odd).astype(m1.dtype)
        first(c, odd, 0).start()

    reduce_neighbours()
    for k in range(FIRST + SUB, PIECES):
        piece(k).start()
    queries[1].wait_recv()
    query_features(1)
    swap_halves()
    send_states(2)
    queries[2].wait_recv()
    query_features(2)
    weights.wait()
    wait_spread(0)
    mix(1, lambda x: sall[0, x])
    neighbour_messages(0, 0)
    wait_spread(1)
    mix(2, lambda x: sall[1, x])
    neighbour_messages(0, 1)

    @pl.loop(1, 4)
    def _(c):
        for odd in range(2):
            neighbour_messages(c, odd)

    take_diagonal()
    reduce_diagonal()
    send_states(3)

    @pl.loop(4, half)
    def _(c):
        for odd in range(2):
            neighbour_messages(c, odd)

    exchange()
    arrived(qin.at[3], qr.at[2])
    query_features(3)
    wait_spread(2)
    mix(3, lambda x: sall[2, x])

    @pl.loop(0, half)
    def _(c):
        for odd in range(2):
            m1[1, c, odd] = times(3, c, odd).astype(m1.dtype)
            first(c, odd, 1).start()

    reduce_own()
    own_query.wait()
    query_features(0)
    mix(0, lambda x: cb[3 * SUB + x])

    for odd in range(2):
        arrived(s2.at[:, odd], t1.at[odd])

    @pl.loop(0, half)
    def _(c):
        for odd in range(2):
            keep[c, odd] = times(0, c, odd) + r1[0, c, odd].astype(jnp.float32)

    @pl.loop(0, half)
    def _(c):
        blocks = [times(1 if odd else 2, c, odd) for odd in range(2)]
        arrived(r1.at[1, c], t1.at[2 + c])
        for odd in range(2):
            s2[c, odd] = (blocks[odd] + r1[1, c, odd].astype(jnp.float32)).astype(s2.dtype)
            second(c, odd).start()

    @pl.loop(0, half)
    def _(c):
        arrived(r2.at[c], s2r.at[c])
        for odd in range(2):
            total = keep[c, odd] + r2[c, odd].astype(jnp.float32)
            out_ref[:, columns(c, odd)] = total.astype(out_ref.dtype)

    arrived(qin.at[pl.ds(0, 3)], qs)
    arrived(up.at[pl.ds(0, SUB + 1)], sts)
    arrived(up.at[pl.ds(0, SUB + NS - 1)], fws)
    arrived(m1, s1)
    arrived(s2, s2s)

    @pl.when(has_inner)
    def _():
        arrived(up, us)

    @pl.when(is_mid)
    def _():
        arrived(up.at[pl.ds(0, 3 * SUB + 2)], us)
        arrived(up.at[pl.ds(0, 2 * SUB + 1)], ds)


def kernel_body(query_rows, key_rows, value_rows, out_weight):
    NS = lax.axis_size("sp")
    _, T, H, size = query_rows.shape
    V, rows = out_weight.shape[1], out_weight.shape[0]
    HD, NC = H // 4, 16
    C, half, count = V // NC, NC // 2, T * NS
    SUB = HD // PART
    G, R = 4 * SUB, PART * size + EXTRA
    bf, f32 = jnp.bfloat16, jnp.float32
    dma = pltpu.SemaphoreType.DMA
    hbm = pl.BlockSpec(memory_space=pl.ANY)
    out = pl.pallas_call(
        functools.partial(kernel, NS, count),
        out_shape=jax.ShapeDtypeStruct((T, V), bf),
        in_specs=[hbm] * 4,
        out_specs=pl.BlockSpec(memory_space=pltpu.VMEM),
        scratch_shapes=[
            pltpu.VMEM((4, 2, T, HD, size), bf),
            pltpu.VMEM((4, T, HD, size), bf),
            pltpu.VMEM((T * HD, size), f32),
            pltpu.VMEM((T * HD, size), f32),
            pltpu.VMEM((rows, V), bf),
            pltpu.VMEM((G, R, size), f32),
            pltpu.VMEM((G, R, size), bf),
            pltpu.VMEM((G, R, size), bf),
            pltpu.VMEM((G, R, size), bf),
            pltpu.VMEM((3, SUB, R, size), bf),
            pltpu.VMEM((4, HD, T, size), bf),
            pltpu.VMEM((4, T, rows), bf),
            pltpu.VMEM((2, half, 2, T, C), bf),
            pltpu.VMEM((2, half, 2, T, C), bf),
            pltpu.VMEM((half, 2, T, C), bf),
            pltpu.VMEM((half, 2, T, C), bf),
            pltpu.VMEM((half, 2, T, C), f32),
            dma((4,)), dma, dma, dma, dma((3,)),
            dma, dma((G,)), dma((G,)), dma, dma, dma, dma((3, SUB)),
            dma, dma((2 + half,)), dma, dma((half,)),
        ],
        compiler_params=pltpu.CompilerParams(
            collective_id=0, has_side_effects=True, vmem_limit_bytes=50 * 2**20
        ),
    )(query_rows[0], key_rows[0], value_rows[0], out_weight)
    return out[None]


def split_of(n):
    for a in range(int(n**0.5), 0, -1):
        if n % a == 0:
            return a, n // a


def body(query_rows, key_rows, value_rows, out_weight):
    ND, NS = lax.axis_size("dp"), lax.axis_size("sp")
    batch, T, H, size = query_rows.shape
    rows, V = out_weight.shape
    fits = batch == 1 and split_of(ND) == (2, 2) and NS == 4 and H // 4 == 4 * PART
    fits = fits and size == 128 and T % 64 == 0 and V % 4096 == 0 and rows * 4 == H * size
    need = 2 * rows * V + 18 * T * V + 12 * T * H * size + 14 * H * size * size
    run = kernel_body if fits and need < 50 * 2**20 else plain_body
    return run(query_rows, key_rows, value_rows, out_weight)


def solution(mesh):
    placed = (
        P(("shift", "dp"), "sp", None, None),
        P(("shift", "dp"), "sp", None, None),
        P(("shift", "dp"), "sp", None, None),
        P(("shift", "dp"), None),
    )
    return jax.shard_map(
        body, mesh=mesh, in_specs=placed, out_specs=P(("shift", "dp"), "sp", None), check_vma=False
    )
```

```python
import functools

import jax
import jax.numpy as jnp
from jax import lax
from jax.experimental import pallas as pl
from jax.experimental.pallas import tpu as pltpu
from jax.sharding import PartitionSpec as P


def feature_map(values):
    wide = values.astype(jnp.float32)
    return jnp.where(wide > 0.0, wide + 1.0, jnp.exp(jnp.minimum(wide, 0.0))).astype(jnp.bfloat16)


def plain_body(query_rows, key_rows, value_rows, out_weight):
    query_feature, key_feature = (feature_map(query_rows), feature_map(key_rows))
    count = query_rows.shape[1] * lax.axis_size("sp")
    state = (
        jnp.einsum("bthd,bthe->bhde", key_feature, value_rows, preferred_element_type=jnp.float32)
        / count
    )
    mass = jnp.sum(key_feature.astype(jnp.float32), axis=1) / count
    state = lax.psum(state.astype(jnp.bfloat16), "sp")
    mass = lax.psum(mass, "sp")
    top = jnp.einsum("bthd,bhde->bthe", query_feature, state, preferred_element_type=jnp.float32)
    bottom = jnp.einsum(
        "bthd,bhd->bth", query_feature.astype(jnp.float32), mass, precision=lax.Precision.HIGHEST
    )
    mixed = (top / (bottom + 0.001)[..., None] * count**0.5).astype(jnp.bfloat16)
    mixed = mixed.reshape(mixed.shape[0], mixed.shape[1], -1)
    mine = lax.all_to_all(mixed, "dp", split_axis=2, concat_axis=0, tiled=True)
    part = jnp.einsum("btw,wv->btv", mine, out_weight, preferred_element_type=jnp.float32)
    return lax.psum_scatter(part.astype(jnp.bfloat16), "dp", scatter_dimension=0, tiled=True)


MESH = pl.DeviceIdType.MESH
NT = (((1,), (1,)), ((), ()))
TN = (((0,), (0,)), ((), ()))
EXTRA = 16
PART = 2


def feature32(values):
    wide = values.astype(jnp.float32)
    return jnp.where(wide > 0.0, wide + 1.0, jnp.exp(jnp.minimum(wide, 0.0)))


def remote(src, dst, send, recv, **where):
    return pltpu.make_async_remote_copy(
        src_ref=src, dst_ref=dst, send_sem=send, recv_sem=recv, device_id=where, device_id_type=MESH
    )


def kernel(
    NS, count, q_hbm, k_hbm, v_hbm, w_hbm, out_ref,
    kv, qin, wide, wide2, w, own, up, inb, cb, sall, qf, mixed,
    m1, r1, s2, r2, keep,
    ksem, lsem, wsem, qs, qr, us, inr, cbr, ds, sts, fws, str_, s1, t1, s2s, s2r,
):
    d, p = lax.axis_index("dp"), lax.axis_index("sp")
    i, j = lax.div(d, 2), lax.rem(d, 2)
    T, HD, size = qin.shape[1:]
    G, SUB = up.shape[0], sall.shape[1]
    C = keep.shape[-1]
    NC = w.shape[1] // C
    mid, half = NS // 2, NC // 2

    def peer(r):
        return lax.rem(i + r // 2, 2) * 2 + lax.rem(j + r % 2, 2)

    side = 1 - lax.div(p, mid)
    center = p - 1 + 2 * side
    outer = p + 1 - 2 * side
    is_mid = jnp.logical_or(p == mid - 1, p == mid)
    has_outer = jnp.logical_and(p > 0, p < NS - 1)
    has_inner = jnp.logical_not(is_mid)
    inside = lax.div(lax.rem(p, NS - 1) + 1, 2)
    mine = inside * (p + 1) + (1 - inside) * lax.div(p, NS - 1)

    for n in range(4):
        rows = pl.ds(peer((n + 1) % 4) * HD, HD)
        pltpu.make_async_copy(k_hbm.at[:, rows], kv.at[n, 0], ksem.at[n]).start()
        pltpu.make_async_copy(v_hbm.at[:, rows], kv.at[n, 1], ksem.at[n]).start()

    barrier = pltpu.get_barrier_semaphore()
    for r in (1, 2, 3):
        pl.semaphore_signal(barrier, inc=1, device_id={"dp": peer(r)}, device_id_type=MESH)
    for x in range(1, NS):
        pl.semaphore_signal(barrier, inc=1, device_id={"sp": lax.rem(p + x, NS)}, device_id_type=MESH)
    PIECES, FIRST = 8, 3

    def piece(k):
        tokens = pl.ds(pl.multiple_of(k * (T // PIECES), T // PIECES), T // PIECES)
        source = q_hbm.at[tokens, pl.ds(peer(3) * HD, HD)]
        return remote(source, qin.at[3, tokens], qs, qr.at[2], dp=peer(3))

    queries = {}
    for r in (1, 2):
        source = q_hbm.at[:, pl.ds(peer(r) * HD, HD)]
        queries[r] = remote(source, qin.at[r], qs, qr.at[r - 1], dp=peer(r))
    own_query = pltpu.make_async_copy(q_hbm.at[:, pl.ds(d * HD, HD)], qin.at[0], lsem)
    weights = pltpu.make_async_copy(w_hbm, w, wsem)

    def widen(src, dst, fn):
        step = 64

        @pl.loop(0, T // step)
        def _(x):
            block = fn(src[pl.ds(pl.multiple_of(x * step, step), step)])
            rows = step * HD
            dst[pl.ds(pl.multiple_of(x * rows, rows), rows)] = block.reshape(rows, size)

    def place(k):
        return (k % 2) * SUB + k // 2

    def up_end(g):
        return remote(up.at[g], inb.at[g], us, inr.at[g], sp=center)

    def up_mid(g):
        return remote(up.at[g], cb.at[g], us, cbr.at[g], sp=center)

    def down(g):
        return remote(cb.at[g], cb.at[g], ds, cbr.at[g], sp=outer)

    def spread(n, x):
        r = n + 1
        dd = (i + r // 2) % 2 * 2 + (j + r) % 2
        return remote(cb.at[n * SUB + x], sall.at[n, x], sts, str_.at[n, x], dp=dd)

    def relay(n, x, to):
        return remote(sall.at[n, x], sall.at[n, x], fws, str_.at[n, x], sp=to)

    def forward(x):
        return remote(sall.at[2, mine], sall.at[2, mine], fws, str_.at[2, mine], sp=lax.rem(p + x, NS))

    for n in range(4):
        pltpu.make_async_copy(kv.at[n], kv.at[n], ksem.at[n]).wait()
        widen(kv.at[n, 0], wide, feature32)
        widen(kv.at[n, 1], wide2, lambda x: x.astype(jnp.float32))

        if n == 0:
            pl.semaphore_wait(barrier, 2 + NS)
            for r in (1, 2):
                queries[r].start()
            for k in range(FIRST):
                piece(k).start()

        @pl.loop(0, SUB)
        def _(x):
            g = n * SUB + x
            row = lax.broadcasted_iota(jnp.int32, (EXTRA, size), 0)
            masses = jnp.zeros((EXTRA, size), jnp.float32)
            for k in range(PART):
                key = wide[pl.ds(x * PART + k, T, stride=HD), :].astype(jnp.bfloat16)
                value = wide2[pl.ds(x * PART + k, T, stride=HD), :].astype(jnp.bfloat16)
                state = lax.dot_general(value, key, TN, preferred_element_type=jnp.float32) / count
                mass = jnp.sum(key.astype(jnp.float32), axis=0, keepdims=True) / count
                masses = jnp.where(row == k, mass, masses)
                own[g, k * size : (k + 1) * size] = state
                up[g, k * size : (k + 1) * size] = state.astype(up.dtype)
            own[g, PART * size :] = masses
            up[g, PART * size :] = masses.astype(up.dtype)

        @pl.when(has_inner)
        def _():
            if n == 0:
                up_end(0).start()
            if n == 1:
                for k in range(1, 2 * SUB):
                    up_end(place(k)).start()
    own_query.start()
    weights.start()

    def take_in(g, both):
        up_end(g).wait_recv()
        total = own[g] + inb[g].astype(jnp.float32)
        keeps = lax.rem(g, 2) == p - 1

        def hold():
            own[g] = total

        def send():
            up[g] = total.astype(up.dtype)
            up_mid(g).start()

        if both:
            hold()
            send()
        else:
            pl.when(keeps)(hold)
            pl.when(jnp.logical_not(keeps))(send)

    def finish(g):
        up_mid(g).wait_recv()
        cb[g] = (own[g] + cb[g].astype(jnp.float32)).astype(cb.dtype)

    LAG = 2

    def reduce_neighbours():
        def step(t, k):
            spread(k % 2, k // 2).start()
            piece(FIRST + t).start()

        @pl.when(is_mid)
        def _():
            for k in range(LAG):
                take_in(place(k), True)

            @pl.loop(0, 2 * SUB)
            def _(k):
                @pl.when(k + LAG < 2 * SUB)
                def _():
                    take_in(place(k + LAG), True)

                finish(place(k))

                @pl.when(k < SUB)
                def _():
                    down(place(k)).start()

                @pl.when(k >= SUB)
                def _():
                    step(k - SUB, k)

        @pl.when(has_inner)
        def _():
            @pl.loop(0, SUB)
            def _(k):
                up_mid(place(k)).wait_recv()
                step(k, k)

    def swap_halves():
        for role, begin, to in ((has_inner, 0, center), (is_mid, SUB, outer)):

            @pl.when(role)
            def _():
                @pl.loop(begin, begin + SUB)
                def _(k):
                    relay(k % 2, k // 2, to).wait_recv()
                    relay(k % 2, k // 2, to).start()

    def take_diagonal():
        @pl.when(is_mid)
        def _():
            @pl.loop(2 * SUB, 3 * SUB)
            def _(g):
                take_in(g, False)

    def reduce_diagonal():
        @pl.when(is_mid)
        def _():
            for x in range(2):
                g = 2 * SUB + 2 * x + p - 1
                finish(g)
                if x == 0:
                    down(g).start()

        @pl.when(has_inner)
        def _():
            up_mid(2 * SUB + mine).wait_recv()

        spread(2, mine).start()

    def send_states(n):
        @pl.when(has_inner)
        def _():
            for g in range(n * SUB, n * SUB + SUB):
                up_end(g).start()

    def reduce_own():
        @pl.when(is_mid)
        def _():
            @pl.loop(3 * SUB, G)
            def _(g):
                take_in(g, True)

            @pl.loop(3 * SUB, G)
            def _(g):
                finish(g)
                down(g).start()

        @pl.when(has_inner)
        def _():
            @pl.loop(3 * SUB, G)
            def _(g):
                up_mid(g).wait_recv()

    def exchange():
        forward(1).wait_recv()
        for x in range(1, NS):
            forward(x).start()

    def query_features(r):
        widen(qin.at[r], wide, feature32)
        for k in range(HD):
            qf[r, k] = wide[pl.ds(k, T, stride=HD), :].astype(qf.dtype)

    def mix(r, states):
        for k in range(HD):
            x, kk = k // PART, k % PART
            block = states(x)
            masses = block[PART * size :].astype(jnp.float32)
            mass = jnp.broadcast_to(masses[kk : kk + 1], (size, size)).astype(jnp.bfloat16)
            both = jnp.concatenate([block[kk * size : (kk + 1) * size], mass], axis=0)
            read = lax.dot_general(qf[r, k], both, NT, preferred_element_type=jnp.float32)
            read = read[:, :size] / (read[:, size:] + 0.001) * count**0.5
            mixed[r, :, k * size : (k + 1) * size] = read.astype(mixed.dtype)

    def wait_spread(n):
        for x in range(SUB):
            if n < 2:
                away = is_mid if x < 2 else has_inner
            else:
                away = x != mine

            @pl.when(away)
            def _():
                spread(n, x).wait_recv()

    def columns(c, odd):
        return pl.ds(pl.multiple_of((2 * c + odd) * C, C), C)

    def first(c, odd, diagonal):
        recv = t1.at[2 + c] if diagonal else t1.at[odd]
        return remote(
            m1.at[diagonal, c, odd], r1.at[diagonal, c, odd], s1, recv, dp=peer(2 if odd else 1)
        )

    def second(c, odd):
        return remote(s2.at[c, odd], r2.at[c, odd], s2s, s2r.at[c], dp=peer(1 if odd else 2))

    def arrived(ref, semaphore):
        pltpu.make_async_copy(ref, ref, semaphore).wait()

    def times(r, c, odd):
        return jnp.dot(mixed[r], w[:, columns(c, odd)], preferred_element_type=jnp.float32)

    def neighbour_messages(c, odd):
        m1[0, c, odd] = times(2 if odd else 1, c, odd).astype(m1.dtype)
        first(c, odd, 0).start()

    reduce_neighbours()
    for k in range(FIRST + SUB, PIECES):
        piece(k).start()
    queries[1].wait_recv()
    query_features(1)
    swap_halves()
    send_states(2)
    queries[2].wait_recv()
    query_features(2)
    weights.wait()
    wait_spread(0)
    mix(1, lambda x: sall[0, x])
    neighbour_messages(0, 0)
    wait_spread(1)
    mix(2, lambda x: sall[1, x])
    neighbour_messages(0, 1)

    @pl.loop(1, 3)
    def _(c):
        for odd in range(2):
            neighbour_messages(c, odd)

    take_diagonal()
    neighbour_messages(3, 0)
    neighbour_messages(3, 1)
    reduce_diagonal()
    send_states(3)

    @pl.loop(4, half)
    def _(c):
        for odd in range(2):
            neighbour_messages(c, odd)

    exchange()
    arrived(qin.at[3], qr.at[2])
    query_features(3)
    wait_spread(2)
    mix(3, lambda x: sall[2, x])

    @pl.loop(0, half)
    def _(c):
        for odd in range(2):
            m1[1, c, odd] = times(3, c, odd).astype(m1.dtype)
            first(c, odd, 1).start()

    reduce_own()
    own_query.wait()
    query_features(0)
    mix(0, lambda x: cb[3 * SUB + x])

    for odd in range(2):
        arrived(s2.at[:, odd], t1.at[odd])

    @pl.loop(0, half)
    def _(c):
        for odd in range(2):
            keep[c, odd] = times(0, c, odd) + r1[0, c, odd].astype(jnp.float32)

    @pl.loop(0, half)
    def _(c):
        blocks = [times(1 if odd else 2, c, odd) for odd in range(2)]
        arrived(r1.at[1, c], t1.at[2 + c])
        for odd in range(2):
            s2[c, odd] = (blocks[odd] + r1[1, c, odd].astype(jnp.float32)).astype(s2.dtype)
            second(c, odd).start()

    @pl.loop(0, half)
    def _(c):
        arrived(r2.at[c], s2r.at[c])
        for odd in range(2):
            total = keep[c, odd] + r2[c, odd].astype(jnp.float32)
            out_ref[:, columns(c, odd)] = total.astype(out_ref.dtype)

    arrived(qin.at[pl.ds(0, 3)], qs)
    arrived(up.at[pl.ds(0, SUB + 1)], sts)
    arrived(up.at[pl.ds(0, SUB + NS - 1)], fws)
    arrived(m1, s1)
    arrived(s2, s2s)

    @pl.when(has_inner)
    def _():
        arrived(up, us)

    @pl.when(is_mid)
    def _():
        arrived(up.at[pl.ds(0, 3 * SUB + 2)], us)
        arrived(up.at[pl.ds(0, 2 * SUB + 1)], ds)


def kernel_body(query_rows, key_rows, value_rows, out_weight):
    NS = lax.axis_size("sp")
    _, T, H, size = query_rows.shape
    V, rows = out_weight.shape[1], out_weight.shape[0]
    HD, NC = H // 4, 16
    C, half, count = V // NC, NC // 2, T * NS
    SUB = HD // PART
    G, R = 4 * SUB, PART * size + EXTRA
    bf, f32 = jnp.bfloat16, jnp.float32
    dma = pltpu.SemaphoreType.DMA
    hbm = pl.BlockSpec(memory_space=pl.ANY)
    out = pl.pallas_call(
        functools.partial(kernel, NS, count),
        out_shape=jax.ShapeDtypeStruct((T, V), bf),
        in_specs=[hbm] * 4,
        out_specs=pl.BlockSpec(memory_space=pltpu.VMEM),
        scratch_shapes=[
            pltpu.VMEM((4, 2, T, HD, size), bf),
            pltpu.VMEM((4, T, HD, size), bf),
            pltpu.VMEM((T * HD, size), f32),
            pltpu.VMEM((T * HD, size), f32),
            pltpu.VMEM((rows, V), bf),
            pltpu.VMEM((G, R, size), f32),
            pltpu.VMEM((G, R, size), bf),
            pltpu.VMEM((G, R, size), bf),
            pltpu.VMEM((G, R, size), bf),
            pltpu.VMEM((3, SUB, R, size), bf),
            pltpu.VMEM((4, HD, T, size), bf),
            pltpu.VMEM((4, T, rows), bf),
            pltpu.VMEM((2, half, 2, T, C), bf),
            pltpu.VMEM((2, half, 2, T, C), bf),
            pltpu.VMEM((half, 2, T, C), bf),
            pltpu.VMEM((half, 2, T, C), bf),
            pltpu.VMEM((half, 2, T, C), f32),
            dma((4,)), dma, dma, dma, dma((3,)),
            dma, dma((G,)), dma((G,)), dma, dma, dma, dma((3, SUB)),
            dma, dma((2 + half,)), dma, dma((half,)),
        ],
        compiler_params=pltpu.CompilerParams(
            collective_id=0, has_side_effects=True, vmem_limit_bytes=50 * 2**20
        ),
    )(query_rows[0], key_rows[0], value_rows[0], out_weight)
    return out[None]


def split_of(n):
    for a in range(int(n**0.5), 0, -1):
        if n % a == 0:
            return a, n // a


def body(query_rows, key_rows, value_rows, out_weight):
    ND, NS = lax.axis_size("dp"), lax.axis_size("sp")
    batch, T, H, size = query_rows.shape
    rows, V = out_weight.shape
    fits = batch == 1 and split_of(ND) == (2, 2) and NS == 4 and H // 4 == 4 * PART
    fits = fits and size == 128 and T % 64 == 0 and V % 4096 == 0 and rows * 4 == H * size
    need = 2 * rows * V + 18 * T * V + 12 * T * H * size + 14 * H * size * size
    run = kernel_body if fits and need < 50 * 2**20 else plain_body
    return run(query_rows, key_rows, value_rows, out_weight)


def solution(mesh):
    placed = (
        P(("shift", "dp"), "sp", None, None),
        P(("shift", "dp"), "sp", None, None),
        P(("shift", "dp"), "sp", None, None),
        P(("shift", "dp"), None),
    )
    return jax.shard_map(
        body, mesh=mesh, in_specs=placed, out_specs=P(("shift", "dp"), "sp", None), check_vma=False
    )
```
